256 devices in a mesh: row: 32 (over y, z_lo, core), col: 8 (over z_hi, x).
Axes of the slice: x: 4, y: 4, z: 8 (z_hi: 2, z_lo: 4; z = z_hi * 4 + z_lo), core: 2. Of those that a mesh axis runs over, the one named last changes fastest.
Arguments:
- left: bfloat16 [16384, 16384], P('row', 'col'), may hold values from -6 to 6
- right: bfloat16 [16384, 16384], P('row', 'col'), may hold values from -0.125 to 0.125
Outputs:
- product: bfloat16 [16384, 16384], P('row', 'col')
The draws below stay inside these ranges and needn't reach their ends.
All inputs are finite; a program needn't handle non-finite values.
Results may differ from the reference program's by a relative error of at most 0.001.
Values may be sent and summed in bfloat16 or wider, within the bound.
A program may use at most 64 MiB of HBM per device.

```python
import jax
import jax.numpy as jnp
from jax import lax

N = 16384
STEPS = 4
GRID = 32
KB = 512


def steps_of(stream_key, shape, split, least, largest):
    factor_of, own = 1.0, jax.random.fold_in(stream_key, 6)
    for axis_at, shards_of in split:
        steps = jnp.exp(jax.random.uniform(jax.random.fold_in(own, axis_at), (shards_of,), jnp.float32, least / len(split), largest / len(split)))
        factor_of = factor_of * jnp.repeat(steps, shape[axis_at] // shards_of).reshape([-1 if axis == axis_at else 1 for axis in range(len(shape))])
    return factor_of


def scatter_about(rng, extent, spread, bound, split=(), kind=jnp.bfloat16):
    result = jax.random.normal(rng, extent, jnp.float32) * spread
    if len(split) > 0:
        result = steps_of(rng, extent, split, -0.22, 0.18) * result
    return jnp.clip(result, min=-bound, max=bound).astype(kind)


def setup_inputs(seed: int = 0) -> dict:
    key_list = jax.random.split(jax.random.key(seed), 3)
    return {
        "left": scatter_about(key_list[0], (N, N), 1.0, 6.0, ((0, 32), (1, 8))),
        "right": scatter_about(key_list[1], (N, N), (STEPS * KB) ** -0.5, 0.125, ((0, 32), (1, 8))),
    }


def reference(left, right):
    def block_row(index):
        total = jnp.zeros((KB, N), jnp.float32)
        for offset in range(STEPS):
            kblock = (index + offset) % GRID
            piece = lax.dynamic_slice(left, (index * KB, kblock * KB), (KB, KB))
            rows = lax.dynamic_slice_in_dim(right, kblock * KB, KB, 0)
            total = total + jnp.dot(piece, rows, preferred_element_type=jnp.float32)
        return total.astype(jnp.bfloat16)

    blocks = lax.map(block_row, jnp.arange(GRID, dtype=jnp.int32))
    return blocks.reshape(N, N)
```

```python
import jax
import jax.numpy as jnp
from jax import lax
from jax.experimental import pallas as pl
from jax.experimental.pallas import tpu as pltpu
from jax.sharding import PartitionSpec as P

MESH = pl.DeviceIdType.MESH
STEPS = 4
CHUNKS = 8
AHEAD = 3
QUARTERS = 4
TOWARDS = (1, 1, -1, -1)
CROSSES = (1, 2, 1, 0)
NEAR = [(s, t) for ts in ((2, 1), (3, 0)) for s in range(STEPS) for t in ts]
FAR = [(s, 3) for s in range(STEPS)] + [(s, t) for s in range(STEPS) for t in (2, 1)] + [(s, 0) for s in range(STEPS)]


def remote(src, dst, sent, got, device):
    return pltpu.make_async_remote_copy(
        src_ref=src, dst_ref=dst, send_sem=sent, recv_sem=got, device_id=device, device_id_type=MESH
    )


def kernel(
    left, right, out, fetched, own, blocks, total, result,
    own_sent, pass_sent, next_sent, next_pass_sent, got, x_sent, cross_sent, piece_got, local, stored,
):
    r, c = lax.axis_index("row"), lax.axis_index("col")
    rows, cols = lax.axis_size("row"), lax.axis_size("col")
    core, q, chips = lax.rem(r, 2), lax.div(r, 2), rows // 2
    ring = cols // 2
    half, x = lax.div(c, ring), lax.rem(c, ring)
    size, width = blocks.shape[1], right.shape[1] // CHUNKS
    tall = size // QUARTERS

    def chip(distance, which):
        return {"row": lax.rem(q + distance + chips, chips) * 2 + which}

    def along(distance):
        return {"col": half * ring + lax.rem(x + distance + ring, ring)}

    across = {"col": (1 - half) * ring + x}
    partner = {"row": q * 2 + 1 - core}

    def columns(i):
        return pl.ds(i * width, width)

    owner, offset = [], []
    for s in range(STEPS):
        owner.append(lax.rem(lax.div(r + s, STEPS), cols))
        offset.append(lax.rem(r + s, STEPS) * size)

    def load_left(s):
        at = pl.ds(pl.multiple_of(offset[s], size), size)
        return pltpu.make_async_copy(left.at[:, at], blocks.at[s], local.at[s])

    load_own = pltpu.make_async_copy(right, own, local.at[STEPS])
    load_own.start()
    for s in range(STEPS):
        @pl.when(c == owner[s])
        def _(s=s):
            load_left(s).start()

    barrier = pltpu.get_barrier_semaphore()
    met = [chip(1, 0), chip(1, 1), chip(-1, 0), chip(-1, 1), partner, along(1), along(-1), across]
    for device in met:
        pl.semaphore_signal(barrier, inc=1, device_id=device, device_id_type=MESH)
    pl.semaphore_wait(barrier, len(met))

    def send_own(i):
        return remote(own.at[:, columns(i)], fetched.at[1, :, columns(i)], own_sent.at[i], got.at[1, i], chip(-1, core))

    def own_to_partner(i):
        return remote(own.at[:, columns(i)], fetched.at[0, :, columns(i)], next_sent.at[i], got.at[0, i], partner)

    def pass_down(i):
        return remote(fetched.at[1, :, columns(i)], fetched.at[2, :, columns(i)], pass_sent.at[i], got.at[2, i], chip(-1, 1))

    def to_partner(i, slot):
        return remote(
            fetched.at[1, :, columns(i)], fetched.at[slot, :, columns(i)], next_pass_sent.at[i], got.at[slot, i], partner
        )

    def place(s, t):
        shift = lax.rem(x - lax.rem(owner[s], ring) + ring, ring)
        hops = shift if TOWARDS[t] > 0 else lax.rem(ring - shift, ring)
        near = half == lax.div(owner[s], ring)
        entered = jnp.where(near, hops, lax.rem(hops - CROSSES[t] + ring, ring))
        return near, hops, entered

    def piece(s, t):
        return blocks.at[s, pl.ds(t * tall, tall), :]

    def send_x(s, t):
        return remote(piece(s, t), piece(s, t), x_sent.at[s, t], piece_got.at[s, t], along(TOWARDS[t]))

    def send_across(s, t):
        return remote(piece(s, t), piece(s, t), cross_sent.at[s, t], piece_got.at[s, t], across)

    def hand_on(s, t, near, hops, entered):
        @pl.when(near & (hops == CROSSES[t]))
        def _():
            send_across(s, t).start()

        @pl.when(entered < ring - 1)
        def _():
            send_x(s, t).start()

    def take(s, t, wanted_near):
        near, hops, entered = place(s, t)

        @pl.when((near == wanted_near) & (jnp.logical_not(near) | (hops > 0)))
        def _():
            send_x(s, t).wait_recv()
            hand_on(s, t, near, hops, entered)

    load_own.wait()
    for i in range(AHEAD):
        send_own(i).start()
    for s in range(STEPS):
        @pl.when(c == owner[s])
        def _(s=s):
            load_left(s).wait()
    for s, t in NEAR:
        near, hops, entered = place(s, t)

        @pl.when(near & (hops == 0))
        def _(s=s, t=t, near=near, hops=hops, entered=entered):
            hand_on(s, t, near, hops, entered)

    @pl.when(core == 1)
    def _():
        for i in range(CHUNKS):
            own_to_partner(i).start()

    per_near, per_far = 4, 2
    for i in range(CHUNKS):
        send_own(i).wait_recv()
        if i + AHEAD < CHUNKS:
            send_own(i + AHEAD).start()

        @pl.when(core == 0)
        def _(i=i):
            to_partner(i, 0).start()
            if i + AHEAD >= CHUNKS:
                pass_down(i + AHEAD - CHUNKS).start()

        @pl.when(core == 1)
        def _(i=i):
            to_partner(i, 2).start()
        for s, t in NEAR[i * per_near : (i + 1) * per_near]:
            take(s, t, True)
        for s, t in FAR[i * per_far : (i + 1) * per_far]:
            take(s, t, False)

    @pl.when(core == 0)
    def _():
        for i in range(AHEAD, CHUNKS):
            pass_down(i).start()

    def dot(s, value):
        return jnp.dot(blocks[s], value, preferred_element_type=jnp.float32)

    @pl.loop(0, CHUNKS)
    def _(i):
        at = pl.ds(pl.multiple_of(i * width, width), width)
        remote(own.at[:, at], fetched.at[0, :, at], own_sent.at[i], got.at[0, i], partner).wait_recv()
        total[:, at] = dot(0, own[:, at]) + dot(1, fetched[0, :, at]) + dot(2, fetched[1, :, at])

    @pl.loop(0, CHUNKS)
    def _(i):
        at = pl.ds(pl.multiple_of(i * width, width), width)
        remote(own.at[:, at], fetched.at[2, :, at], own_sent.at[i], got.at[2, i], partner).wait_recv()
        result[:, at] = (total[:, at] + dot(3, fetched[2, :, at])).astype(result.dtype)
        pltpu.make_async_copy(result.at[:, at], out.at[:, at], stored.at[i]).start()

    for i in range(CHUNKS):
        send_own(i).wait_send()
        to_partner(i, 0).wait_send()

        @pl.when(core == 0)
        def _(i=i):
            pass_down(i).wait_send()

        @pl.when(core == 1)
        def _(i=i):
            own_to_partner(i).wait_send()
    for s in range(STEPS):
        for t in range(QUARTERS):
            near, hops, entered = place(s, t)

            @pl.when(near & (hops == CROSSES[t]))
            def _(s=s, t=t):
                send_across(s, t).wait_send()

            @pl.when(entered < ring - 1)
            def _(s=s, t=t):
                send_x(s, t).wait_send()
    for i in range(CHUNKS):
        pltpu.make_async_copy(result.at[:, columns(i)], out.at[:, columns(i)], stored.at[i]).wait()


def local(left, right):
    size, width = right.shape
    dma = pltpu.SemaphoreType.DMA
    return pl.pallas_call(
        kernel,
        out_shape=jax.ShapeDtypeStruct((size, width), jnp.bfloat16),
        in_specs=[pl.BlockSpec(memory_space=pl.ANY)] * 2,
        out_specs=pl.BlockSpec(memory_space=pl.ANY),
        scratch_shapes=[
            pltpu.VMEM((STEPS - 1, size, width), jnp.bfloat16),
            pltpu.VMEM((size, width), jnp.bfloat16),
            pltpu.VMEM((STEPS, size, size), jnp.bfloat16),
            pltpu.VMEM((size, width), jnp.float32),
            pltpu.VMEM((size, width), jnp.bfloat16),
            dma((CHUNKS,)), dma((CHUNKS,)), dma((CHUNKS,)), dma((CHUNKS,)), dma((STEPS - 1, CHUNKS)),
            dma((STEPS, QUARTERS)), dma((STEPS, QUARTERS)), dma((STEPS, QUARTERS)), dma((STEPS + 1,)), dma((CHUNKS,)),
        ],
        compiler_params=pltpu.CompilerParams(collective_id=0, has_side_effects=True, vmem_limit_bytes=56 * 2**20),
    )(left, right)


def solution(mesh):
    return jax.shard_map(
        local,
        mesh=mesh,
        in_specs=(P("row", "col"), P("row", "col")),
        out_specs=P("row", "col"),
        check_vma=False,
    )
```

```python
import jax
import jax.numpy as jnp
from jax import lax
from jax.experimental import pallas as pl
from jax.experimental.pallas import tpu as pltpu
from jax.sharding import PartitionSpec as P

MESH = pl.DeviceIdType.MESH
STEPS = 4
RUN = 4
CHUNKS = 8
AHEAD = 4
QUARTERS = 4
NEAR = (0, 1, 2, 3)
FAR = (3, 4, 5, 6)
RELAY = (2, 3, 4, 5)


def remote(src, dst, sent, got, device):
    return pltpu.make_async_remote_copy(
        src_ref=src, dst_ref=dst, send_sem=sent, recv_sem=got, device_id=device, device_id_type=MESH
    )


def kernel(
    left, right, out, fetched, own, blocks, total, result,
    own_sent, pass_sent, next_sent, next_pass_sent, got, x_sent, scatter_sent, cross_sent, piece_got, local, stored,
    transit, transit_got, relay_sent, closing_sent,
):
    r, c = lax.axis_index("row"), lax.axis_index("col")
    rows, cols = lax.axis_size("row"), lax.axis_size("col")
    core, q, chips = lax.rem(r, 2), lax.div(r, 2), rows // 2
    ring = cols // 2
    half, x = lax.div(c, ring), lax.rem(c, ring)
    size, width = blocks.shape[1], right.shape[1] // CHUNKS
    tall = size // QUARTERS

    def chip(distance, which):
        return {"row": lax.rem(q + distance + chips, chips) * 2 + which}

    def along(distance):
        return {"col": half * ring + lax.rem(x + distance + ring, ring)}

    across = {"col": (1 - half) * ring + x}
    along_z = lax.rem(q, RUN)
    ends = jnp.logical_or(along_z == 0, along_z == RUN - 1)
    relayed = jnp.logical_and(ends, core == 1)
    other_end = jnp.where(along_z == 0, r + 2 * (RUN - 1), jnp.where(along_z == RUN - 1, r - 2 * (RUN - 1), r))
    partner = {"row": q * 2 + 1 - core}

    def columns(i):
        return pl.ds(i * width, width)

    owner, offset = [], []
    for s in range(STEPS):
        owner.append(lax.rem(lax.div(r + s, STEPS), cols))
        offset.append(lax.rem(r + s, STEPS) * size)

    def load_left(s):
        at = pl.ds(pl.multiple_of(offset[s], size), size)
        return pltpu.make_async_copy(left.at[:, at], blocks.at[s], local.at[s])

    load_own = pltpu.make_async_copy(right, own, local.at[STEPS])
    load_own.start()
    for s in range(STEPS):
        @pl.when(c == owner[s])
        def _(s=s):
            load_left(s).start()

    barrier = pltpu.get_barrier_semaphore()
    met = [partner, along(1), along(2), along(3), across]
    first, last = along_z == 0, along_z == RUN - 1
    leaps_down = jnp.logical_and(along_z <= 1, core == 0)
    leaps_up = jnp.logical_and(along_z >= RUN - 2, core == 1)
    groups = [
        (jnp.logical_not(first), [chip(-1, 0), chip(-1, 1)]),
        (jnp.logical_not(last), [chip(1, 0), chip(1, 1)]),
        (leaps_down, [chip(-2, 1)]),
        (leaps_up, [chip(2, 0)]),
        (jnp.logical_and(first, core == 1), [chip(-1, 1)]),
        (jnp.logical_and(last, core == 1), [chip(1, 1)]),
        (relayed, [{"row": other_end}, {"row": other_end, **across}]),
    ]
    expected = len(met)
    for needed, devices in groups:
        expected = expected + jnp.where(needed, len(devices), 0)

        @pl.when(needed)
        def _(devices=devices):
            for device in devices:
                pl.semaphore_signal(barrier, inc=1, device_id=device, device_id_type=MESH)
    for device in met:
        pl.semaphore_signal(barrier, inc=1, device_id=device, device_id_type=MESH)
    pl.semaphore_wait(barrier, expected)

    relays_right = jnp.logical_and(along_z == RUN - 2, core == 1)
    skips = jnp.logical_and(first, core == 0)
    below = {"row": jnp.where(skips, chip(-2, 1)["row"], chip(-1, core)["row"])}
    below_slot = jnp.where(skips, 2, 1)

    def send_own(i):
        return remote(
            own.at[:, columns(i)], fetched.at[below_slot, :, columns(i)], own_sent.at[i], got.at[below_slot, i], below
        )

    def next_two(i):
        return remote(own.at[:, columns(i)], fetched.at[1, :, columns(i)], own_sent.at[i], got.at[1, i], partner)

    def closing(i):
        return remote(
            fetched.at[2, :, columns(i)], fetched.at[1, :, columns(i)], closing_sent.at[i], got.at[1, i], chip(1, 0)
        )

    def closing_in(i):
        return remote(own.at[:, columns(i)], fetched.at[2, :, columns(i)], own_sent.at[i], got.at[2, i], partner)

    def leap(i):
        return remote(own.at[:, columns(i)], fetched.at[2, :, columns(i)], closing_sent.at[i], got.at[2, i], chip(-2, 1))

    leaps = jnp.logical_and(along_z == 1, core == 0)
    passes = jnp.logical_and(jnp.logical_or(along_z == 1, along_z == 2), core == 0)

    def own_to_partner(i):
        return remote(own.at[:, columns(i)], fetched.at[0, :, columns(i)], next_sent.at[i], got.at[0, i], partner)

    def pass_down(i):
        return remote(fetched.at[1, :, columns(i)], fetched.at[2, :, columns(i)], pass_sent.at[i], got.at[2, i], chip(-1, 1))

    def to_partner(i, slot):
        return remote(
            fetched.at[1, :, columns(i)], fetched.at[slot, :, columns(i)], next_pass_sent.at[i], got.at[slot, i], partner
        )

    def root(s):
        return lax.rem(owner[s], ring), half == lax.div(owner[s], ring)

    def piece(s, t):
        return blocks.at[s, pl.ds(pl.multiple_of(t * tall, tall), tall), :]

    def line(s, t, d, device):
        return remote(piece(s, t), piece(s, t), x_sent.at[s, d], piece_got.at[s, t], device)

    def scatter(s, d):
        return remote(
            piece(s, lax.rem(x + d, ring)), piece(s, lax.rem(x + d, ring)),
            scatter_sent.at[s, d], piece_got.at[s, lax.rem(x + d, ring)], along(d),
        )

    def gather(s, d):
        return line(s, x, d, along(d))

    def send_across(s):
        return remote(piece(s, x), piece(s, x), cross_sent.at[s], piece_got.at[s, x], across)

    def send_to_relay(s):
        return remote(piece(s, x), transit.at[s], cross_sent.at[s], transit_got.at[s], {"row": other_end, **across})

    def relay(s):
        return remote(transit.at[s], piece(s, x), relay_sent.at[s], piece_got.at[s, x], {"row": other_end})

    def relays(s):
        from_half = lax.div(lax.rem(lax.div(other_end + s, STEPS), cols), ring)
        return jnp.logical_and(relayed, half != from_half)

    def hand_on(s):
        @pl.when(relays(s))
        def _():
            send_to_relay(s).wait_recv()
            relay(s).start()

    def wants(s, d):
        at, near = root(s)
        return jnp.logical_not(near & (lax.rem(x + d, ring) == at))

    def is_root(s):
        return c == owner[s]

    def share(s):
        at, near = root(s)

        @pl.when(jnp.logical_and(near, jnp.logical_not(relayed)))
        def _():
            send_across(s).start()

        @pl.when(jnp.logical_and(near, relayed))
        def _():
            send_to_relay(s).start()
        for d in (1, 3, 2):
            @pl.when(wants(s, d))
            def _(d=d):
                gather(s, d).start()

    def take(s, wanted_near):
        at, near = root(s)

        @pl.when((near == wanted_near) & jnp.logical_not(is_root(s)))
        def _():
            gather(s, 1).wait_recv()
            share(s)

    load_own.wait()
    for i in range(AHEAD):
        send_own(i).start()
    for s in range(STEPS):
        @pl.when(c == owner[s])
        def _(s=s):
            load_left(s).wait()
    for s in range(STEPS):
        @pl.when(is_root(s))
        def _(s=s):
            for d in (2, 1, 3):
                scatter(s, d).start()
    for s in range(STEPS):
        @pl.when(is_root(s))
        def _(s=s):
            share(s)

    @pl.when(core == 1)
    def _():
        for i in range(CHUNKS):
            own_to_partner(i).start()

    for i in range(CHUNKS):
        send_own(i).wait_send()
        if i + AHEAD < CHUNKS:
            send_own(i + AHEAD).start()

        @pl.when(jnp.logical_not(last))
        def _(i=i):
            next_two(i).wait_recv()
            to_partner(i, 2 * core).start()

        @pl.when(relays_right)
        def _(i=i):
            closing_in(i).wait_recv()
            closing(i).start()
        if i >= CHUNKS // 2:
            @pl.when(leaps)
            def _(i=i):
                for j in range(2 * i - CHUNKS, 2 * i - CHUNKS + 2):
                    leap(j).start()
        if i + AHEAD >= CHUNKS:
            @pl.when(passes)
            def _(i=i):
                pass_down(i + AHEAD - CHUNKS).start()
        for s in range(STEPS):
            if NEAR[s] == i:
                take(s, True)
            if FAR[s] == i:
                take(s, False)
            if RELAY[s] == i:
                hand_on(s)

    @pl.when(passes)
    def _():
        for i in range(AHEAD, CHUNKS):
            pass_down(i).start()

    def await_left(s):
        @pl.when(jnp.logical_not(is_root(s)))
        def _():
            for d in range(1, ring):
                line(s, lax.rem(x + d, ring), d, along(d)).wait_recv()

    def window(i):
        return pl.ds(pl.multiple_of(i * width, width), width)

    def await_right(slot, i):
        remote(own.at[:, window(i)], fetched.at[slot, :, window(i)], own_sent.at[i], got.at[slot, i], partner).wait_recv()

    def dot(s, value):
        return jnp.dot(blocks[s], value, preferred_element_type=jnp.float32)

    def finish(i, summed):
        result[:, window(i)] = summed.astype(result.dtype)
        pltpu.make_async_copy(result.at[:, window(i)], out.at[:, window(i)], stored.at[i]).start()

    await_left(0)

    @pl.loop(0, CHUNKS)
    def _(i):
        total[:, window(i)] = dot(0, own[:, window(i)])

    @pl.when(jnp.logical_not(last))
    def _():
        for s in range(1, STEPS - 1):
            await_left(s)

            @pl.loop(0, CHUNKS)
            def _(i, s=s):
                if s == 1:
                    await_right(0, i)
                total[:, window(i)] += dot(s, fetched[s - 1, :, window(i)])

        await_left(STEPS - 1)

        @pl.loop(0, CHUNKS)
        def _(i):
            @pl.when(jnp.logical_not(relays_right))
            def _():
                await_right(STEPS - 2, i)
            finish(i, total[:, window(i)] + dot(STEPS - 1, fetched[STEPS - 2, :, window(i)]))

    @pl.when(last)
    def _():
        def forward(i):
            await_right(1, i)
            remote(
                fetched.at[1, :, window(i)], fetched.at[2 * core, :, window(i)],
                next_pass_sent.at[i], got.at[2 * core, i], partner,
            ).start()

        for s in range(1, STEPS):
            await_left(s)
        forward(0)

        @pl.loop(0, CHUNKS)
        def _(i):
            @pl.when(i + 1 < CHUNKS)
            def _():
                forward(i + 1)
            await_right(0, i)
            await_right(2, i)
            summed = total[:, window(i)]
            for s in range(1, STEPS):
                summed += dot(s, fetched[s - 1, :, window(i)])
            finish(i, summed)

    for i in range(CHUNKS):
        to_partner(i, 0).wait_send()

        @pl.when(passes)
        def _(i=i):
            pass_down(i).wait_send()

        @pl.when(jnp.logical_or(relays_right, leaps))
        def _(i=i):
            leap(i).wait_send()

        @pl.when(core == 1)
        def _(i=i):
            own_to_partner(i).wait_send()
    for s in range(STEPS):
        at, near = root(s)

        @pl.when(near)
        def _(s=s):
            send_across(s).wait_send()

        @pl.when(relays(s))
        def _(s=s):
            relay(s).wait_send()
        for d in range(1, ring):
            @pl.when(wants(s, d))
            def _(s=s, d=d):
                gather(s, d).wait_send()

            @pl.when(is_root(s))
            def _(s=s, d=d):
                scatter(s, d).wait_send()
    for i in range(CHUNKS):
        pltpu.make_async_copy(result.at[:, columns(i)], out.at[:, columns(i)], stored.at[i]).wait()


def local(left, right):
    size, width = right.shape
    dma = pltpu.SemaphoreType.DMA
    return pl.pallas_call(
        kernel,
        out_shape=jax.ShapeDtypeStruct((size, width), jnp.bfloat16),
        in_specs=[pl.BlockSpec(memory_space=pl.ANY)] * 2,
        out_specs=pl.BlockSpec(memory_space=pl.ANY),
        scratch_shapes=[
            pltpu.VMEM((STEPS - 1, size, width), jnp.bfloat16),
            pltpu.VMEM((size, width), jnp.bfloat16),
            pltpu.VMEM((STEPS, size, size), jnp.bfloat16),
            pltpu.VMEM((size, width), jnp.float32),
            pltpu.VMEM((size, width), jnp.bfloat16),
            dma((CHUNKS,)), dma((CHUNKS,)), dma((CHUNKS,)), dma((CHUNKS,)), dma((STEPS - 1, CHUNKS)),
            dma((STEPS, QUARTERS)), dma((STEPS, QUARTERS)), dma((STEPS,)), dma((STEPS, QUARTERS)), dma((STEPS + 1,)), dma((CHUNKS,)),
            pltpu.VMEM((STEPS, size // QUARTERS, size), jnp.bfloat16), dma((STEPS,)), dma((STEPS,)), dma((CHUNKS,)),
        ],
        compiler_params=pltpu.CompilerParams(collective_id=0, has_side_effects=True, vmem_limit_bytes=56 * 2**20),
    )(left, right)


def solution(mesh):
    return jax.shard_map(
        local,
        mesh=mesh,
        in_specs=(P("row", "col"), P("row", "col")),
        out_specs=P("row", "col"),
        check_vma=False,
    )
```

```python
import jax
import jax.numpy as jnp
from jax import lax
from jax.experimental import pallas as pl
from jax.experimental.pallas import tpu as pltpu
from jax.sharding import PartitionSpec as P

MESH = pl.DeviceIdType.MESH
STEPS = 4
FIRST_MORE, LAST_MORE = 2, 0
EARLY = 2
RUN = 4
CHUNKS = 8
PER = 1
AHEAD = 4
QUARTERS = 4
NEAR = (0, 1, 2, 3)
FAR = (3, 4, 5, 6)
RELAY = (2, 3, 4, 5)


def remote(src, dst, sent, got, device):
    return pltpu.make_async_remote_copy(
        src_ref=src, dst_ref=dst, send_sem=sent, recv_sem=got, device_id=device, device_id_type=MESH
    )


def kernel(
    left, right, out, fetched, own, blocks, total,
    own_sent, pass_sent, next_sent, next_pass_sent, got, x_sent, scatter_sent, cross_sent, piece_got, local,
    transit, transit_got, relay_sent, closing_sent,
):
    r, c = lax.axis_index("row"), lax.axis_index("col")
    rows, cols = lax.axis_size("row"), lax.axis_size("col")
    core, q, chips = lax.rem(r, 2), lax.div(r, 2), rows // 2
    ring = cols // 2
    half, x = lax.div(c, ring), lax.rem(c, ring)
    size, width = blocks.shape[1], right.shape[1] // CHUNKS
    tall = size // QUARTERS

    def chip(distance, which):
        return {"row": lax.rem(q + distance + chips, chips) * 2 + which}

    def along(distance):
        return {"col": half * ring + lax.rem(x + distance + ring, ring)}

    across = {"col": (1 - half) * ring + x}
    along_z = lax.rem(q, RUN)
    ends = jnp.logical_or(along_z == 0, along_z == RUN - 1)

    def crosses_by_relay(s, at_first):
        return jnp.logical_or(core == 1, s < jnp.where(at_first, FIRST_MORE, LAST_MORE))

    def relayed(s):
        return jnp.logical_and(ends, crosses_by_relay(s, along_z == 0))
    other_end = jnp.where(along_z == 0, r + 2 * (RUN - 1), jnp.where(along_z == RUN - 1, r - 2 * (RUN - 1), r))
    partner = {"row": q * 2 + 1 - core}

    def columns(i):
        return pl.ds(i * width, width)

    owner, offset = [], []
    for s in range(STEPS):
        owner.append(lax.rem(lax.div(r + s, STEPS), cols))
        offset.append(lax.rem(r + s, STEPS) * size)

    def load_left(s):
        at = pl.ds(pl.multiple_of(offset[s], size), size)
        return pltpu.make_async_copy(left.at[:, at], blocks.at[s], local.at[s])

    load_own = pltpu.make_async_copy(right, own, local.at[STEPS])
    load_own.start()
    for s in range(STEPS):
        @pl.when(c == owner[s])
        def _(s=s):
            load_left(s).start()

    barrier = pltpu.get_barrier_semaphore()
    met = [partner, along(1), along(2), along(3), across]
    first, last = along_z == 0, along_z == RUN - 1
    leaps_down = jnp.logical_and(along_z <= 1, core == 0)
    leaps_up = jnp.logical_and(along_z >= RUN - 2, core == 1)
    groups = [
        (jnp.logical_not(first), [chip(-1, 0), chip(-1, 1)]),
        (jnp.logical_not(last), [chip(1, 0), chip(1, 1)]),
        (leaps_down, [chip(-2, 1)]),
        (leaps_up, [chip(2, 0)]),
        (jnp.logical_and(first, core == 1), [chip(-1, 1)]),
        (jnp.logical_and(last, core == 1), [chip(1, 1)]),
        (ends, [{"row": other_end}, {"row": other_end, **across}]),
    ]
    expected = len(met)
    for needed, devices in groups:
        expected = expected + jnp.where(needed, len(devices), 0)

        @pl.when(needed)
        def _(devices=devices):
            for device in devices:
                pl.semaphore_signal(barrier, inc=1, device_id=device, device_id_type=MESH)
    for device in met:
        pl.semaphore_signal(barrier, inc=1, device_id=device, device_id_type=MESH)
    pl.semaphore_wait(barrier, expected)

    relays_right = jnp.logical_and(along_z == RUN - 2, core == 1)
    skips = jnp.logical_and(first, core == 0)
    below = {"row": jnp.where(skips, chip(-2, 1)["row"], chip(-1, core)["row"])}
    below_slot = jnp.where(skips, 2, 1)

    def send_own(i):
        return remote(
            own.at[:, columns(i)], fetched.at[below_slot, :, columns(i)], own_sent.at[i], got.at[below_slot, i], below
        )

    def next_two(i):
        return remote(own.at[:, columns(i)], fetched.at[1, :, columns(i)], own_sent.at[i], got.at[1, i], partner)

    def closing(i):
        return remote(
            fetched.at[2, :, columns(i)], fetched.at[1, :, columns(i)], closing_sent.at[i], got.at[1, i], chip(1, 0)
        )

    def closing_in(i):
        return remote(own.at[:, columns(i)], fetched.at[2, :, columns(i)], own_sent.at[i], got.at[2, i], partner)

    def leap(i):
        return remote(own.at[:, columns(i)], fetched.at[2, :, columns(i)], closing_sent.at[i], got.at[2, i], chip(-2, 1))

    leaps = jnp.logical_and(along_z == 1, core == 0)
    passes = jnp.logical_and(jnp.logical_or(along_z == 1, along_z == 2), core == 0)

    def own_to_partner(i):
        return remote(own.at[:, columns(i)], fetched.at[0, :, columns(i)], next_sent.at[i], got.at[0, i], partner)

    def pass_down(i):
        return remote(fetched.at[1, :, columns(i)], fetched.at[2, :, columns(i)], pass_sent.at[i], got.at[2, i], chip(-1, 1))

    def to_partner(i, slot):
        return remote(
            fetched.at[1, :, columns(i)], fetched.at[slot, :, columns(i)], next_pass_sent.at[i], got.at[slot, i], partner
        )

    def root(s):
        return lax.rem(owner[s], ring), half == lax.div(owner[s], ring)

    def piece(s, t):
        return blocks.at[s, pl.ds(pl.multiple_of(t * tall, tall), tall), :]

    def line(s, t, d, device):
        return remote(piece(s, t), piece(s, t), x_sent.at[s, d], piece_got.at[s, t], device)

    def scatter(s, d):
        return remote(
            piece(s, lax.rem(x + d, ring)), piece(s, lax.rem(x + d, ring)),
            scatter_sent.at[s, d], piece_got.at[s, lax.rem(x + d, ring)], along(d),
        )

    def gather(s, d):
        return line(s, x, d, along(d))

    def send_across(s):
        return remote(piece(s, x), piece(s, x), cross_sent.at[s], piece_got.at[s, x], across)

    def send_to_relay(s):
        return remote(piece(s, x), transit.at[s], cross_sent.at[s], transit_got.at[s], {"row": other_end, **across})

    def relay(s):
        return remote(transit.at[s], piece(s, x), relay_sent.at[s], piece_got.at[s, x], {"row": other_end})

    def relays(s):
        from_half = lax.div(lax.rem(lax.div(other_end + s, STEPS), cols), ring)
        return jnp.logical_and(jnp.logical_and(ends, crosses_by_relay(s, last)), half != from_half)

    def hand_on(s):
        @pl.when(relays(s))
        def _():
            send_to_relay(s).wait_recv()
            relay(s).start()

    def wants(s, d):
        at, near = root(s)
        return jnp.logical_not(near & (lax.rem(x + d, ring) == at))

    def is_root(s):
        return c == owner[s]

    def share(s):
        at, near = root(s)

        @pl.when(jnp.logical_and(near, jnp.logical_not(relayed(s))))
        def _():
            send_across(s).start()

        @pl.when(jnp.logical_and(near, relayed(s)))
        def _():
            send_to_relay(s).start()
        for d in (1, 3, 2):
            @pl.when(wants(s, d))
            def _(d=d):
                gather(s, d).start()

    def take(s, wanted_near):
        at, near = root(s)

        @pl.when((near == wanted_near) & jnp.logical_not(is_root(s)))
        def _():
            gather(s, 1).wait_recv()
            share(s)

    load_own.wait()
    for i in range(AHEAD):
        send_own(i).start()

    @pl.when(leaps)
    def _():
        for i in range(EARLY):
            leap(i).start()
    for s in range(STEPS):
        @pl.when(c == owner[s])
        def _(s=s):
            load_left(s).wait()
    for s in range(STEPS):
        @pl.when(is_root(s))
        def _(s=s):
            for d in (2, 1, 3):
                scatter(s, d).start()
    for s in range(STEPS):
        @pl.when(is_root(s))
        def _(s=s):
            share(s)

    @pl.when(core == 1)
    def _():
        for i in range(CHUNKS):
            own_to_partner(i).start()

    for i in range(CHUNKS):
        send_own(i).wait_send()
        if i + AHEAD < CHUNKS:
            send_own(i + AHEAD).start()

        @pl.when(jnp.logical_not(last))
        def _(i=i):
            next_two(i).wait_recv()
            to_partner(i, 2 * core).start()

        @pl.when(relays_right)
        def _(i=i):
            closing_in(i).wait_recv()
            closing(i).start()
        if i >= CHUNKS // 2:
            @pl.when(leaps)
            def _(i=i):
                for j in range(max(EARLY, 2 * i - CHUNKS), 2 * i - CHUNKS + 2):
                    leap(j).start()
        if i + AHEAD >= CHUNKS:
            @pl.when(passes)
            def _(i=i):
                pass_down(i + AHEAD - CHUNKS).start()
        for s in range(STEPS):
            if NEAR[s] * PER + PER - 1 == i:
                take(s, True)
            if FAR[s] * PER + PER - 1 == i:
                take(s, False)
            if RELAY[s] * PER + PER - 1 == i:
                hand_on(s)

    @pl.when(passes)
    def _():
        for i in range(AHEAD, CHUNKS):
            pass_down(i).start()

    def await_left(s):
        @pl.when(jnp.logical_not(is_root(s)))
        def _():
            for d in range(1, ring):
                line(s, lax.rem(x + d, ring), d, along(d)).wait_recv()

    def window(i):
        return pl.ds(pl.multiple_of(i * (PER * width), PER * width), PER * width)

    def chunk(i):
        return pl.ds(pl.multiple_of(i * width, width), width)

    def await_right(slot, i):
        for j in range(PER):
            at, n = chunk(i * PER + j), i * PER + j
            remote(own.at[:, at], fetched.at[slot, :, at], own_sent.at[n], got.at[slot, n], partner).wait_recv()

    def dot(s, value):
        return jnp.dot(blocks[s], value, preferred_element_type=jnp.float32)

    def finish(i, summed):
        out[:, window(i)] = summed.astype(out.dtype)

    await_left(0)

    @pl.loop(0, CHUNKS // PER)
    def _(i):
        total[:, window(i)] = dot(0, own[:, window(i)])

    @pl.when(jnp.logical_not(last))
    def _():
        for s in range(1, STEPS - 1):
            await_left(s)

            @pl.loop(0, CHUNKS // PER)
            def _(i, s=s):
                if s == 1:
                    await_right(0, i)
                total[:, window(i)] += dot(s, fetched[s - 1, :, window(i)])

        await_left(STEPS - 1)

        @pl.loop(0, CHUNKS // PER)
        def _(i):
            @pl.when(jnp.logical_not(relays_right))
            def _():
                await_right(STEPS - 2, i)
            finish(i, total[:, window(i)] + dot(STEPS - 1, fetched[STEPS - 2, :, window(i)]))

    @pl.when(last)
    def _():
        def forward(i):
            await_right(1, i)
            for j in range(PER):
                at, n = chunk(i * PER + j), i * PER + j
                remote(
                    fetched.at[1, :, at], fetched.at[2 * core, :, at], next_pass_sent.at[n], got.at[2 * core, n], partner
                ).start()

        for s in range(1, STEPS):
            await_left(s)
        forward(0)

        @pl.loop(0, CHUNKS // PER)
        def _(i):
            @pl.when(i + 1 < CHUNKS // PER)
            def _():
                forward(i + 1)
            await_right(0, i)
            await_right(2, i)
            summed = total[:, window(i)]
            for s in range(1, STEPS):
                summed += dot(s, fetched[s - 1, :, window(i)])
            finish(i, summed)

    for i in range(CHUNKS):
        to_partner(i, 0).wait_send()

        @pl.when(passes)
        def _(i=i):
            pass_down(i).wait_send()

        @pl.when(jnp.logical_or(relays_right, leaps))
        def _(i=i):
            leap(i).wait_send()

        @pl.when(core == 1)
        def _(i=i):
            own_to_partner(i).wait_send()
    for s in range(STEPS):
        at, near = root(s)

        @pl.when(near)
        def _(s=s):
            send_across(s).wait_send()

        @pl.when(relays(s))
        def _(s=s):
            relay(s).wait_send()
        for d in range(1, ring):
            @pl.when(wants(s, d))
            def _(s=s, d=d):
                gather(s, d).wait_send()

            @pl.when(is_root(s))
            def _(s=s, d=d):
                scatter(s, d).wait_send()


def local(left, right):
    size, width = right.shape
    dma = pltpu.SemaphoreType.DMA
    return pl.pallas_call(
        kernel,
        out_shape=jax.ShapeDtypeStruct((size, width), jnp.bfloat16),
        in_specs=[pl.BlockSpec(memory_space=pltpu.HBM)] * 2,
        out_specs=pl.BlockSpec(memory_space=pltpu.VMEM),
        scratch_shapes=[
            pltpu.VMEM((STEPS - 1, size, width), jnp.bfloat16),
            pltpu.VMEM((size, width), jnp.bfloat16),
            pltpu.VMEM((STEPS, size, size), jnp.bfloat16),
            pltpu.VMEM((size, width), jnp.float32),
            dma((CHUNKS,)), dma((CHUNKS,)), dma((CHUNKS,)), dma((CHUNKS,)), dma((STEPS - 1, CHUNKS)),
            dma((STEPS, QUARTERS)), dma((STEPS, QUARTERS)), dma((STEPS,)), dma((STEPS, QUARTERS)), dma((STEPS + 1,)),
            pltpu.VMEM((STEPS, size // QUARTERS, size), jnp.bfloat16), dma((STEPS,)), dma((STEPS,)), dma((CHUNKS,)),
        ],
        compiler_params=pltpu.CompilerParams(collective_id=0, has_side_effects=True, vmem_limit_bytes=20 * 2**20),
    )(pltpu.with_memory_space_constraint(left, pltpu.HBM), pltpu.with_memory_space_constraint(right, pltpu.HBM))


def solution(mesh):
    return jax.shard_map(
        local,
        mesh=mesh,
        in_specs=(P("row", "col"), P("row", "col")),
        out_specs=P("row", "col"),
        check_vma=False,
    )
```

```python
import jax
import jax.numpy as jnp
from jax import lax
from jax.experimental import pallas as pl
from jax.experimental.pallas import tpu as pltpu
from jax.sharding import PartitionSpec as P

MESH = pl.DeviceIdType.MESH
STEPS = 4
FIRST_MORE, LAST_MORE = 1, 1
THIRD = 2
EARLY = 2
RUN = 4
CHUNKS = 8
PER = 1
AHEAD = 4
QUARTERS = 4
NEAR = (0, 1, 2, 3)
FAR = (7, 7, 7, 7)
RELAY = (2, 3, 4, 5)


def remote(src, dst, sent, got, device):
    return pltpu.make_async_remote_copy(
        src_ref=src, dst_ref=dst, send_sem=sent, recv_sem=got, device_id=device, device_id_type=MESH
    )


def kernel(
    left, right, out, fetched, own, blocks, total,
    own_sent, pass_sent, next_sent, next_pass_sent, got, x_sent, scatter_sent, cross_sent, piece_got, local,
    transit, transit_got, relay_sent, closing_sent,
):
    r, c = lax.axis_index("row"), lax.axis_index("col")
    rows, cols = lax.axis_size("row"), lax.axis_size("col")
    core, q, chips = lax.rem(r, 2), lax.div(r, 2), rows // 2
    ring = cols // 2
    half, x = lax.div(c, ring), lax.rem(c, ring)
    size, width = blocks.shape[1], right.shape[1] // CHUNKS
    tall = size // QUARTERS

    def chip(distance, which):
        return {"row": lax.rem(q + distance + chips, chips) * 2 + which}

    def along(distance):
        return {"col": half * ring + lax.rem(x + distance + ring, ring)}

    across = {"col": (1 - half) * ring + x}
    along_z = lax.rem(q, RUN)
    ends = jnp.logical_or(along_z == 0, along_z == RUN - 1)

    def crosses_by_relay(s, position):
        at_end = jnp.logical_or(core == 1, s < jnp.where(position == 0, FIRST_MORE, LAST_MORE))
        at_third = jnp.logical_and(core == 1, s < THIRD)
        return jnp.where(position == RUN - 2, at_third, jnp.logical_and(position != 1, at_end))

    def relayed(s):
        return crosses_by_relay(s, along_z)

    mate = r + 2 * jnp.where(ends, jnp.where(along_z == 0, RUN - 1, 1 - RUN), jnp.where(along_z == 1, 1, -1))
    partner = {"row": q * 2 + 1 - core}

    def columns(i):
        return pl.ds(i * width, width)

    owner, offset = [], []
    for s in range(STEPS):
        owner.append(lax.rem(lax.div(r + s, STEPS), cols))
        offset.append(lax.rem(r + s, STEPS) * size)

    def load_left(s):
        at = pl.ds(pl.multiple_of(offset[s], size), size)
        return pltpu.make_async_copy(left.at[:, at], blocks.at[s], local.at[s])

    load_own = pltpu.make_async_copy(right, own, local.at[STEPS])
    load_own.start()
    for s in range(STEPS):
        @pl.when(c == owner[s])
        def _(s=s):
            load_left(s).start()

    barrier = pltpu.get_barrier_semaphore()
    met = [partner, along(1), along(2), along(3), across]
    first, last = along_z == 0, along_z == RUN - 1
    leaps_down = jnp.logical_and(along_z <= 1, core == 0)
    leaps_up = jnp.logical_and(along_z >= RUN - 2, core == 1)
    groups = [
        (jnp.logical_not(first), [chip(-1, 0), chip(-1, 1)]),
        (jnp.logical_not(last), [chip(1, 0), chip(1, 1)]),
        (leaps_down, [chip(-2, 1)]),
        (leaps_up, [chip(2, 0)]),
        (jnp.logical_and(first, core == 1), [chip(-1, 1)]),
        (jnp.logical_and(last, core == 1), [chip(1, 1)]),
        (ends, [{"row": mate}]),
        (jnp.logical_or(ends, core == 1), [{"row": mate, **across}]),
    ]
    expected = len(met)
    for needed, devices in groups:
        expected = expected + jnp.where(needed, len(devices), 0)

        @pl.when(needed)
        def _(devices=devices):
            for device in devices:
                pl.semaphore_signal(barrier, inc=1, device_id=device, device_id_type=MESH)
    for device in met:
        pl.semaphore_signal(barrier, inc=1, device_id=device, device_id_type=MESH)
    pl.semaphore_wait(barrier, expected)

    relays_right = jnp.logical_and(along_z == RUN - 2, core == 1)
    skips = jnp.logical_and(first, core == 0)
    below = {"row": jnp.where(skips, chip(-2, 1)["row"], chip(-1, core)["row"])}
    below_slot = jnp.where(skips, 2, 1)

    def send_own(i):
        return remote(
            own.at[:, columns(i)], fetched.at[below_slot, :, columns(i)], own_sent.at[i], got.at[below_slot, i], below
        )

    def next_two(i):
        return remote(own.at[:, columns(i)], fetched.at[1, :, columns(i)], own_sent.at[i], got.at[1, i], partner)

    def closing(i):
        return remote(
            fetched.at[2, :, columns(i)], fetched.at[1, :, columns(i)], closing_sent.at[i], got.at[1, i], chip(1, 0)
        )

    def closing_in(i):
        return remote(own.at[:, columns(i)], fetched.at[2, :, columns(i)], own_sent.at[i], got.at[2, i], partner)

    def leap(i):
        return remote(own.at[:, columns(i)], fetched.at[2, :, columns(i)], closing_sent.at[i], got.at[2, i], chip(-2, 1))

    leaps = jnp.logical_and(along_z == 1, core == 0)
    passes = jnp.logical_and(jnp.logical_or(along_z == 1, along_z == 2), core == 0)

    def own_to_partner(i):
        return remote(own.at[:, columns(i)], fetched.at[0, :, columns(i)], next_sent.at[i], got.at[0, i], partner)

    def pass_down(i):
        return remote(fetched.at[1, :, columns(i)], fetched.at[2, :, columns(i)], pass_sent.at[i], got.at[2, i], chip(-1, 1))

    def to_partner(i, slot):
        return remote(
            fetched.at[1, :, columns(i)], fetched.at[slot, :, columns(i)], next_pass_sent.at[i], got.at[slot, i], partner
        )

    def root(s):
        return lax.rem(owner[s], ring), half == lax.div(owner[s], ring)

    def piece(s, t):
        return blocks.at[s, pl.ds(pl.multiple_of(t * tall, tall), tall), :]

    def line(s, t, d, device):
        return remote(piece(s, t), piece(s, t), x_sent.at[s, d], piece_got.at[s, t], device)

    def scatter(s, d):
        return remote(
            piece(s, lax.rem(x + d, ring)), piece(s, lax.rem(x + d, ring)),
            scatter_sent.at[s, d], piece_got.at[s, lax.rem(x + d, ring)], along(d),
        )

    def gather(s, d):
        return line(s, x, d, along(d))

    def send_across(s):
        return remote(piece(s, x), piece(s, x), cross_sent.at[s], piece_got.at[s, x], across)

    near_mate = {"row": mate, "col": jnp.where(ends, across["col"], c)}
    far_mate = {"row": mate, "col": jnp.where(ends, c, across["col"])}

    def send_to_relay(s):
        return remote(piece(s, x), transit.at[s], cross_sent.at[s], transit_got.at[s], near_mate)

    def relay(s):
        return remote(transit.at[s], piece(s, x), relay_sent.at[s], piece_got.at[s, x], far_mate)

    def relays(s):
        from_half = lax.div(lax.rem(lax.div(mate + s, STEPS), cols), ring)
        position = lax.rem(lax.div(mate, 2), RUN)
        placed = jnp.where(ends, half != from_half, half == from_half)
        return jnp.logical_and(crosses_by_relay(s, position), placed)

    def hand_on(s):
        @pl.when(relays(s))
        def _():
            send_to_relay(s).wait_recv()
            relay(s).start()

    def wants(s, d):
        at, near = root(s)
        return jnp.logical_not(near & (lax.rem(x + d, ring) == at))

    def is_root(s):
        return c == owner[s]

    def share(s):
        at, near = root(s)

        @pl.when(jnp.logical_and(near, jnp.logical_not(relayed(s))))
        def _():
            send_across(s).start()

        @pl.when(jnp.logical_and(near, relayed(s)))
        def _():
            send_to_relay(s).start()
        for d in (1, 3, 2):
            @pl.when(wants(s, d))
            def _(d=d):
                gather(s, d).start()

    def take(s, wanted_near):
        at, near = root(s)

        @pl.when((near == wanted_near) & jnp.logical_not(is_root(s)))
        def _():
            gather(s, 1).wait_recv()
            share(s)

    load_own.wait()
    for i in range(AHEAD):
        send_own(i).start()

    @pl.when(leaps)
    def _():
        for i in range(EARLY):
            leap(i).start()
    for s in range(STEPS):
        @pl.when(c == owner[s])
        def _(s=s):
            load_left(s).wait()
    for s in range(STEPS):
        @pl.when(is_root(s))
        def _(s=s):
            for d in (2, 1, 3):
                scatter(s, d).start()
    for s in range(STEPS):
        @pl.when(is_root(s))
        def _(s=s):
            share(s)

    @pl.when(core == 1)
    def _():
        for i in range(CHUNKS):
            own_to_partner(i).start()

    for i in range(CHUNKS):
        send_own(i).wait_send()
        if i + AHEAD < CHUNKS:
            send_own(i + AHEAD).start()

        @pl.when(jnp.logical_not(last))
        def _(i=i):
            next_two(i).wait_recv()
            to_partner(i, 2 * core).start()

        @pl.when(relays_right)
        def _(i=i):
            closing_in(i).wait_recv()
            closing(i).start()
        if i >= CHUNKS // 2:
            @pl.when(leaps)
            def _(i=i):
                for j in range(max(EARLY, 2 * i - CHUNKS), 2 * i - CHUNKS + 2):
                    leap(j).start()
        if i >= CHUNKS // 2:
            @pl.when(passes)
            def _(i=i):
                for j in range(2 * i - CHUNKS, 2 * i - CHUNKS + 2):
                    pass_down(j).start()
        for s in range(STEPS):
            if NEAR[s] * PER + PER - 1 == i:
                take(s, True)
            if FAR[s] * PER + PER - 1 == i:
                take(s, False)
            if RELAY[s] * PER + PER - 1 == i:
                hand_on(s)


    def await_left(s):
        @pl.when(jnp.logical_not(is_root(s)))
        def _():
            for d in range(1, ring):
                line(s, lax.rem(x + d, ring), d, along(d)).wait_recv()

    def window(i):
        return pl.ds(pl.multiple_of(i * (PER * width), PER * width), PER * width)

    def chunk(i):
        return pl.ds(pl.multiple_of(i * width, width), width)

    def await_right(slot, i):
        for j in range(PER):
            at, n = chunk(i * PER + j), i * PER + j
            remote(own.at[:, at], fetched.at[slot, :, at], own_sent.at[n], got.at[slot, n], partner).wait_recv()

    def dot(s, value):
        return jnp.dot(blocks[s], value, preferred_element_type=jnp.float32)

    def left_is_sent():
        for s in range(STEPS):
            at, near = root(s)

            @pl.when(near)
            def _(s=s):
                send_across(s).wait_send()

            @pl.when(relays(s))
            def _(s=s):
                relay(s).wait_send()
            for d in range(1, ring):
                @pl.when(wants(s, d))
                def _(s=s, d=d):
                    gather(s, d).wait_send()

                @pl.when(is_root(s))
                def _(s=s, d=d):
                    scatter(s, d).wait_send()

    def finish(i, summed):
        out[:, window(i)] = summed.astype(out.dtype)

    await_left(0)

    @pl.loop(0, CHUNKS // PER)
    def _(i):
        total[:, window(i)] = dot(0, own[:, window(i)])

    @pl.when(jnp.logical_not(last))
    def _():
        for s in range(1, STEPS - 1):
            await_left(s)

            @pl.loop(0, CHUNKS // PER)
            def _(i, s=s):
                if s == 1:
                    await_right(0, i)
                total[:, window(i)] += dot(s, fetched[s - 1, :, window(i)])

        await_left(STEPS - 1)
        left_is_sent()
        for i in range(CHUNKS):
            to_partner(i, 0).wait_send()

        @pl.loop(0, CHUNKS // PER)
        def _(i):
            @pl.when(jnp.logical_not(relays_right))
            def _():
                await_right(STEPS - 2, i)
            finish(i, total[:, window(i)] + dot(STEPS - 1, fetched[STEPS - 2, :, window(i)]))

    @pl.when(last)
    def _():
        def forward(i):
            await_right(1, i)
            for j in range(PER):
                at, n = chunk(i * PER + j), i * PER + j
                remote(
                    fetched.at[1, :, at], fetched.at[2 * core, :, at], next_pass_sent.at[n], got.at[2 * core, n], partner
                ).start()

        for s in range(1, STEPS):
            await_left(s)
        forward(0)
        left_is_sent()

        @pl.loop(0, CHUNKS // PER)
        def _(i):
            @pl.when(i + 1 < CHUNKS // PER)
            def _():
                forward(i + 1)
            await_right(0, i)
            await_right(2, i)
            summed = total[:, window(i)]
            for s in range(1, STEPS):
                summed += dot(s, fetched[s - 1, :, window(i)])
            finish(i, summed)

    for i in range(CHUNKS):
        @pl.when(last)
        def _(i=i):
            to_partner(i, 0).wait_send()

        @pl.when(passes)
        def _(i=i):
            pass_down(i).wait_send()

        @pl.when(jnp.logical_or(relays_right, leaps))
        def _(i=i):
            leap(i).wait_send()

        @pl.when(core == 1)
        def _(i=i):
            own_to_partner(i).wait_send()


def local(left, right):
    size, width = right.shape
    dma = pltpu.SemaphoreType.DMA
    return pl.pallas_call(
        kernel,
        out_shape=jax.ShapeDtypeStruct((size, width), jnp.bfloat16),
        in_specs=[pl.BlockSpec(memory_space=pltpu.HBM)] * 2,
        out_specs=pl.BlockSpec(memory_space=pltpu.VMEM),
        scratch_shapes=[
            pltpu.VMEM((STEPS - 1, size, width), jnp.bfloat16),
            pltpu.VMEM((size, width), jnp.bfloat16),
            pltpu.VMEM((STEPS, size, size), jnp.bfloat16),
            pltpu.VMEM((size, width), jnp.float32),
            dma((CHUNKS,)), dma((CHUNKS,)), dma((CHUNKS,)), dma((CHUNKS,)), dma((STEPS - 1, CHUNKS)),
            dma((STEPS, QUARTERS)), dma((STEPS, QUARTERS)), dma((STEPS,)), dma((STEPS, QUARTERS)), dma((STEPS + 1,)),
            pltpu.VMEM((STEPS, size // QUARTERS, size), jnp.bfloat16), dma((STEPS,)), dma((STEPS,)), dma((CHUNKS,)),
        ],
        compiler_params=pltpu.CompilerParams(collective_id=0, has_side_effects=True, vmem_limit_bytes=20 * 2**20),
    )(pltpu.with_memory_space_constraint(left, pltpu.HBM), pltpu.with_memory_space_constraint(right, pltpu.HBM))


def solution(mesh):
    return jax.shard_map(
        local,
        mesh=mesh,
        in_specs=(P("row", "col"), P("row", "col")),
        out_specs=P("row", "col"),
        check_vma=False,
    )
```

```python
import jax
import jax.numpy as jnp
from jax import lax
from jax.experimental import pallas as pl
from jax.experimental.pallas import tpu as pltpu
from jax.sharding import PartitionSpec as P

MESH = pl.DeviceIdType.MESH
STEPS = 4
FIRST_MORE, LAST_MORE = 1, 1
THIRD = 2
EARLY = 2
RUN = 4
CHUNKS = 8
PER = 1
AHEAD = 4
QUARTERS = 4
NEAR = (0, 1, 2, 3)
FAR = (7, 7, 7, 7)
RELAY = (1, 2, 3, 4)


def remote(src, dst, sent, got, device):
    return pltpu.make_async_remote_copy(
        src_ref=src, dst_ref=dst, send_sem=sent, recv_sem=got, device_id=device, device_id_type=MESH
    )


def kernel(
    left, right, out, fetched, own, blocks, total,
    own_sent, pass_sent, next_sent, next_pass_sent, got, x_sent, scatter_sent, cross_sent, piece_got, local,
    transit, transit_got, relay_sent, closing_sent,
):
    r, c = lax.axis_index("row"), lax.axis_index("col")
    rows, cols = lax.axis_size("row"), lax.axis_size("col")
    core, q, chips = lax.rem(r, 2), lax.div(r, 2), rows // 2
    ring = cols // 2
    half, x = lax.div(c, ring), lax.rem(c, ring)
    size, width = blocks.shape[1], right.shape[1] // CHUNKS
    tall = size // QUARTERS

    def chip(distance, which):
        return {"row": lax.rem(q + distance + chips, chips) * 2 + which}

    def along(distance):
        return {"col": half * ring + lax.rem(x + distance + ring, ring)}

    across = {"col": (1 - half) * ring + x}
    along_z = lax.rem(q, RUN)
    ends = jnp.logical_or(along_z == 0, along_z == RUN - 1)

    def crosses_by_relay(s, position):
        at_end = jnp.logical_or(core == 1, s < jnp.where(position == 0, FIRST_MORE, LAST_MORE))
        at_third = jnp.logical_and(core == 1, s < THIRD)
        return jnp.where(position == RUN - 2, at_third, jnp.logical_and(position != 1, at_end))

    def relayed(s):
        return crosses_by_relay(s, along_z)

    mate = r + 2 * jnp.where(ends, jnp.where(along_z == 0, RUN - 1, 1 - RUN), jnp.where(along_z == 1, 1, -1))
    partner = {"row": q * 2 + 1 - core}

    def columns(i):
        return pl.ds(i * width, width)

    owner, offset = [], []
    for s in range(STEPS):
        owner.append(lax.rem(lax.div(r + s, STEPS), cols))
        offset.append(lax.rem(r + s, STEPS) * size)

    def load_left(s):
        at = pl.ds(pl.multiple_of(offset[s], size), size)
        return pltpu.make_async_copy(left.at[:, at], blocks.at[s], local.at[s])

    load_own = pltpu.make_async_copy(right, own, local.at[STEPS])
    load_own.start()
    for s in range(STEPS):
        @pl.when(c == owner[s])
        def _(s=s):
            load_left(s).start()

    barrier = pltpu.get_barrier_semaphore()
    met = [partner, along(1), along(2), along(3), across]
    first, last = along_z == 0, along_z == RUN - 1
    leaps_down = jnp.logical_and(along_z <= 1, core == 0)
    leaps_up = jnp.logical_and(along_z >= RUN - 2, core == 1)
    groups = [
        (jnp.logical_not(first), [chip(-1, 0), chip(-1, 1)]),
        (jnp.logical_not(last), [chip(1, 0), chip(1, 1)]),
        (leaps_down, [chip(-2, 1)]),
        (leaps_up, [chip(2, 0)]),
        (jnp.logical_and(first, core == 1), [chip(-1, 1)]),
        (jnp.logical_and(last, core == 1), [chip(1, 1)]),
        (ends, [{"row": mate}]),
        (jnp.logical_or(ends, core == 1), [{"row": mate, **across}]),
    ]
    expected = len(met)
    for needed, devices in groups:
        expected = expected + jnp.where(needed, len(devices), 0)

        @pl.when(needed)
        def _(devices=devices):
            for device in devices:
                pl.semaphore_signal(barrier, inc=1, device_id=device, device_id_type=MESH)
    for device in met:
        pl.semaphore_signal(barrier, inc=1, device_id=device, device_id_type=MESH)
    pl.semaphore_wait(barrier, expected)

    relays_right = jnp.logical_and(along_z == RUN - 2, core == 1)
    skips = jnp.logical_and(first, core == 0)
    below = {"row": jnp.where(skips, chip(-2, 1)["row"], chip(-1, core)["row"])}
    below_slot = jnp.where(skips, 2, 1)

    def send_own(i):
        return remote(
            own.at[:, columns(i)], fetched.at[below_slot, :, columns(i)], own_sent.at[i], got.at[below_slot, i], below
        )

    def next_two(i):
        return remote(own.at[:, columns(i)], fetched.at[1, :, columns(i)], own_sent.at[i], got.at[1, i], partner)

    def closing(i):
        return remote(
            fetched.at[2, :, columns(i)], fetched.at[1, :, columns(i)], closing_sent.at[i], got.at[1, i], chip(1, 0)
        )

    def closing_in(i):
        return remote(own.at[:, columns(i)], fetched.at[2, :, columns(i)], own_sent.at[i], got.at[2, i], partner)

    def leap(i):
        return remote(own.at[:, columns(i)], fetched.at[2, :, columns(i)], closing_sent.at[i], got.at[2, i], chip(-2, 1))

    leaps = jnp.logical_and(along_z == 1, core == 0)
    passes = jnp.logical_and(jnp.logical_or(along_z == 1, along_z == 2), core == 0)

    def own_to_partner(i):
        return remote(own.at[:, columns(i)], fetched.at[0, :, columns(i)], next_sent.at[i], got.at[0, i], partner)

    def pass_down(i):
        return remote(fetched.at[1, :, columns(i)], fetched.at[2, :, columns(i)], pass_sent.at[i], got.at[2, i], chip(-1, 1))

    def to_partner(i, slot):
        return remote(
            fetched.at[1, :, columns(i)], fetched.at[slot, :, columns(i)], next_pass_sent.at[i], got.at[slot, i], partner
        )

    def root(s):
        return lax.rem(owner[s], ring), half == lax.div(owner[s], ring)

    def piece(s, t):
        return blocks.at[s, pl.ds(pl.multiple_of(t * tall, tall), tall), :]

    def line(s, t, d, device):
        return remote(piece(s, t), piece(s, t), x_sent.at[s, d], piece_got.at[s, t], device)

    def scatter(s, d):
        return remote(
            piece(s, lax.rem(x + d, ring)), piece(s, lax.rem(x + d, ring)),
            scatter_sent.at[s, d], piece_got.at[s, lax.rem(x + d, ring)], along(d),
        )

    def gather(s, d):
        return line(s, x, d, along(d))

    def send_across(s):
        return remote(piece(s, x), piece(s, x), cross_sent.at[s], piece_got.at[s, x], across)

    near_mate = {"row": mate, "col": jnp.where(ends, across["col"], c)}
    far_mate = {"row": mate, "col": jnp.where(ends, c, across["col"])}

    def send_to_relay(s):
        return remote(piece(s, x), transit.at[s], cross_sent.at[s], transit_got.at[s], near_mate)

    def relay(s):
        return remote(transit.at[s], piece(s, x), relay_sent.at[s], piece_got.at[s, x], far_mate)

    def relays(s):
        from_half = lax.div(lax.rem(lax.div(mate + s, STEPS), cols), ring)
        position = lax.rem(lax.div(mate, 2), RUN)
        placed = jnp.where(ends, half != from_half, half == from_half)
        return jnp.logical_and(crosses_by_relay(s, position), placed)

    def hand_on(s):
        @pl.when(relays(s))
        def _():
            send_to_relay(s).wait_recv()
            relay(s).start()

    def wants(s, d):
        at, near = root(s)
        return jnp.logical_not(near & (lax.rem(x + d, ring) == at))

    def is_root(s):
        return c == owner[s]

    def share(s):
        at, near = root(s)

        @pl.when(jnp.logical_and(near, jnp.logical_not(relayed(s))))
        def _():
            send_across(s).start()

        @pl.when(jnp.logical_and(near, relayed(s)))
        def _():
            send_to_relay(s).start()
        for d in (1, 3, 2):
            @pl.when(wants(s, d))
            def _(d=d):
                gather(s, d).start()

    def take(s, wanted_near):
        at, near = root(s)

        @pl.when((near == wanted_near) & jnp.logical_not(is_root(s)))
        def _():
            gather(s, 1).wait_recv()
            share(s)

    load_own.wait()
    for i in range(AHEAD):
        send_own(i).start()

    @pl.when(leaps)
    def _():
        for i in range(EARLY):
            leap(i).start()
    for s in range(STEPS):
        @pl.when(c == owner[s])
        def _(s=s):
            load_left(s).wait()
    for s in range(STEPS):
        @pl.when(is_root(s))
        def _(s=s):
            for d in (2, 1, 3):
                scatter(s, d).start()
    for s in range(STEPS):
        @pl.when(is_root(s))
        def _(s=s):
            share(s)

    @pl.when(core == 1)
    def _():
        for i in range(CHUNKS):
            own_to_partner(i).start()

    for i in range(CHUNKS):
        send_own(i).wait_send()
        if i + AHEAD < CHUNKS:
            send_own(i + AHEAD).start()

        @pl.when(jnp.logical_not(last))
        def _(i=i):
            next_two(i).wait_recv()
            to_partner(i, 2 * core).start()

        @pl.when(relays_right)
        def _(i=i):
            closing_in(i).wait_recv()
            closing(i).start()
        if i >= CHUNKS // 2:
            @pl.when(leaps)
            def _(i=i):
                for j in range(max(EARLY, 2 * i - CHUNKS), 2 * i - CHUNKS + 2):
                    leap(j).start()
        if i >= CHUNKS // 2:
            @pl.when(passes)
            def _(i=i):
                for j in range(2 * i - CHUNKS, 2 * i - CHUNKS + 2):
                    pass_down(j).start()
        for s in range(STEPS):
            if NEAR[s] * PER + PER - 1 == i:
                take(s, True)
            if FAR[s] * PER + PER - 1 == i:
                take(s, False)
            if RELAY[s] * PER + PER - 1 == i:
                hand_on(s)


    def await_left(s):
        @pl.when(jnp.logical_not(is_root(s)))
        def _():
            for d in range(1, ring):
                line(s, lax.rem(x + d, ring), d, along(d)).wait_recv()

    def window(i):
        return pl.ds(pl.multiple_of(i * (PER * width), PER * width), PER * width)

    def chunk(i):
        return pl.ds(pl.multiple_of(i * width, width), width)

    def await_right(slot, i):
        for j in range(PER):
            at, n = chunk(i * PER + j), i * PER + j
            remote(own.at[:, at], fetched.at[slot, :, at], own_sent.at[n], got.at[slot, n], partner).wait_recv()

    def dot(s, value):
        return jnp.dot(blocks[s], value, preferred_element_type=jnp.float32)

    def left_is_sent():
        for s in range(STEPS):
            at, near = root(s)

            @pl.when(near)
            def _(s=s):
                send_across(s).wait_send()

            @pl.when(relays(s))
            def _(s=s):
                relay(s).wait_send()
            for d in range(1, ring):
                @pl.when(wants(s, d))
                def _(s=s, d=d):
                    gather(s, d).wait_send()

                @pl.when(is_root(s))
                def _(s=s, d=d):
                    scatter(s, d).wait_send()

    def finish(i, summed):
        out[:, window(i)] = summed.astype(out.dtype)

    await_left(0)

    @pl.loop(0, CHUNKS // PER)
    def _(i):
        total[:, window(i)] = dot(0, own[:, window(i)])

    @pl.when(jnp.logical_not(last))
    def _():
        for s in range(1, STEPS - 1):
            await_left(s)

            @pl.loop(0, CHUNKS // PER)
            def _(i, s=s):
                if s == 1:
                    await_right(0, i)
                total[:, window(i)] += dot(s, fetched[s - 1, :, window(i)])

        await_left(STEPS - 1)
        left_is_sent()
        for i in range(CHUNKS):
            to_partner(i, 0).wait_send()

        @pl.loop(0, CHUNKS // PER)
        def _(i):
            @pl.when(jnp.logical_not(relays_right))
            def _():
                await_right(STEPS - 2, i)
            finish(i, total[:, window(i)] + dot(STEPS - 1, fetched[STEPS - 2, :, window(i)]))

    @pl.when(last)
    def _():
        def forward(i):
            await_right(1, i)
            for j in range(PER):
                at, n = chunk(i * PER + j), i * PER + j
                remote(
                    fetched.at[1, :, at], fetched.at[2 * core, :, at], next_pass_sent.at[n], got.at[2 * core, n], partner
                ).start()

        for s in range(1, STEPS):
            await_left(s)
        forward(0)
        left_is_sent()

        @pl.loop(0, CHUNKS // PER)
        def _(i):
            @pl.when(i + 1 < CHUNKS // PER)
            def _():
                forward(i + 1)
            await_right(0, i)
            await_right(2, i)
            summed = total[:, window(i)]
            for s in range(1, STEPS):
                summed += dot(s, fetched[s - 1, :, window(i)])
            finish(i, summed)

    for i in range(CHUNKS):
        @pl.when(last)
        def _(i=i):
            to_partner(i, 0).wait_send()

        @pl.when(passes)
        def _(i=i):
            pass_down(i).wait_send()

        @pl.when(jnp.logical_or(relays_right, leaps))
        def _(i=i):
            leap(i).wait_send()

        @pl.when(core == 1)
        def _(i=i):
            own_to_partner(i).wait_send()


def local(left, right):
    size, width = right.shape
    dma = pltpu.SemaphoreType.DMA
    return pl.pallas_call(
        kernel,
        out_shape=jax.ShapeDtypeStruct((size, width), jnp.bfloat16),
        in_specs=[pl.BlockSpec(memory_space=pltpu.HBM)] * 2,
        out_specs=pl.BlockSpec(memory_space=pltpu.VMEM),
        scratch_shapes=[
            pltpu.VMEM((STEPS - 1, size, width), jnp.bfloat16),
            pltpu.VMEM((size, width), jnp.bfloat16),
            pltpu.VMEM((STEPS, size, size), jnp.bfloat16),
            pltpu.VMEM((size, width), jnp.float32),
            dma((CHUNKS,)), dma((CHUNKS,)), dma((CHUNKS,)), dma((CHUNKS,)), dma((STEPS - 1, CHUNKS)),
            dma((STEPS, QUARTERS)), dma((STEPS, QUARTERS)), dma((STEPS,)), dma((STEPS, QUARTERS)), dma((STEPS + 1,)),
            pltpu.VMEM((STEPS, size // QUARTERS, size), jnp.bfloat16), dma((STEPS,)), dma((STEPS,)), dma((CHUNKS,)),
        ],
        compiler_params=pltpu.CompilerParams(collective_id=0, has_side_effects=True, vmem_limit_bytes=20 * 2**20),
    )(pltpu.with_memory_space_constraint(left, pltpu.HBM), pltpu.with_memory_space_constraint(right, pltpu.HBM))


def solution(mesh):
    return jax.shard_map(
        local,
        mesh=mesh,
        in_specs=(P("row", "col"), P("row", "col")),
        out_specs=P("row", "col"),
        check_vma=False,
    )
```
